768 devices in a mesh: pp: 12 (over z), tp: 16 (over y, core), ep: 4 (over x).
Axes of the slice: x: 4, y: 8, z: 12, core: 2. Of those that a mesh axis runs over, the one named last changes fastest.
Arguments:
- incoming: bfloat16 [12, 8192, 2048], P('pp', ('tp', 'ep')), may hold values from -6 to 6
- expert_ids: int32 [12, 8192, 2], P('pp', ('tp', 'ep')), may hold values from 0 to 63, all different within a row; in each aligned block of 128 rows (0 to 127, 128 to 255, ..., all dimensions but the last counted through in order) at most 8 rows name the same one
- gate_scores: float32 [12, 8192, 2], P('pp', ('tp', 'ep')), may hold values from 0.05 to 1
- gate_proj: bfloat16 [64, 2048, 768], P(('tp', 'ep')), may hold values from -0.125 to 0.125
- up_proj: bfloat16 [64, 2048, 768], P(('tp', 'ep')), may hold values from -0.125 to 0.125
- down_proj: bfloat16 [64, 768, 2048], P(('tp', 'ep')), may hold values from -0.21875 to 0.21875
Outputs:
- combined: bfloat16 [12, 8192, 2048], P('pp', ('tp', 'ep'))
The draws below stay inside these ranges and needn't reach their ends.
Inputs may be any that keep to these rules, and one draw needn't show every extreme that they name: `expert_ids`: each token names 2 different experts. Among the tokens of one device of one section no expert is named more than 8 times, and in every draw some device's tokens name one expert exactly 8 times.
All inputs are finite; a program needn't handle non-finite values.
Results may differ from the reference program's by a relative error of at most 0.0045.
Values may be sent and summed in bfloat16 or wider, within the bound.
No kernel may reach another device: no remote copies, remote signals or barrier semaphores. Data moves between devices by JAX's collectives and lax.ppermute only.
A program may use at most 64 MiB of HBM per device.

```python
import math
import jax
import jax.numpy as jnp
import numpy as np
from jax import lax

D = 2048
FF = 768
TOPK = 2
TOK_DEV = 128
EXPERTS = 64
CAP = 8
TOKENS = 8192
N_PP = 12
N_TP = 16
N_EP = 4


def steps_of(own_key, shape, pieces, low, high):
    def one(axis_at, shards_of):
        steps = jax.random.uniform(jax.random.fold_in(jax.random.fold_in(own_key, 6), axis_at), (shards_of,), jnp.float32, low / len(pieces), high / len(pieces))
        return jnp.repeat(jnp.exp(steps), shape[axis_at] // shards_of).reshape((-1,) + (1,) * (len(shape) - axis_at - 1))

    level = one(*pieces[0])
    for cut in pieces[1:]:
        level = level * one(*cut)
    return level


def deal_out(key, own, number, rows, number_of, top, most, slope):
    sequence = jax.random.permutation(key, number_of)
    heavy_load, ordinary = portions_of(number_of, rows * top, most, slope, True), portions_of(number_of, rows * top, most, slope, False)
    places = jnp.arange(number_of)

    def named(sizes, turn):
        used = int((sizes > 0).sum())
        fixed = max(1, used // 4)
        shifted = fixed + (places - fixed + turn * (used - fixed)) % max(1, number_of - fixed)
        return jnp.zeros((number_of,), jnp.int32).at[sequence[jnp.where(places < fixed, places, shifted)]].set(jnp.asarray(sizes, jnp.int32))

    sizes = jnp.where(number % 4 == 0, named(heavy_load, number // 4), named(ordinary, number - number // 4 - 1))
    mixed = jax.random.permutation(jax.random.fold_in(own, 3), number_of)
    source_of, taker = mixed[0:number_of // 2 * 2:2], mixed[1:number_of // 2 * 2:2]
    margin = jnp.minimum(sizes[source_of] - 1, most - sizes[taker]) // 2
    margin = jnp.where((source_of == sequence[0]) | (taker == sequence[0]) | (sizes[taker] == 0), 0, jnp.maximum(margin, 0))
    shifted = jax.random.randint(jax.random.fold_in(own, 4), (number_of // 2,), 0, 1 << 20) % (margin + 1)
    sizes = sizes.at[source_of].add(-shifted).at[taker].add(shifted)
    members = jnp.searchsorted(jnp.cumsum(sizes), jnp.arange(rows * top), side="right").astype(jnp.int32)
    table = members.reshape(top, rows).T
    table = table[jax.random.permutation(jax.random.fold_in(own, 1), rows)]
    turn = jax.random.randint(jax.random.fold_in(own, 2), (rows, 1), 0, top)
    return jnp.take_along_axis(table, (jnp.arange(top)[None, :] + turn) % top, axis=1)


def portions_of(amount, total, most, slope, full):
    portions = [(1 << 20) // math.isqrt(rank ** slope) + 1 for rank in range(1, amount + 1)]
    largest = most if full else min(most, max(-(-total // amount), total * portions[0] // sum(portions)))
    least = 1 if total - largest >= amount - 1 else 0
    holding, rest = [largest] + [least] * (amount - 1), total - largest - least * (amount - 1)
    while rest > 0:
        movable = [i for i in range(1, amount) if holding[i] < largest] or [i for i in range(1, amount) if holding[i] < most]
        pool, budget = sum([portions[i] for i in movable]), rest
        for i in movable:
            addition = min(most - holding[i], max(1, budget * portions[i] // pool), rest)
            holding[i] = holding[i] + addition
            rest = rest - addition
    return np.array(holding)


def noise(key, shape, deviation, most, split=(), kind=jnp.bfloat16):
    loudness = steps_of(key, shape, split, -0.22, 0.18) if split else 1.0
    values = jax.random.normal(key, shape, jnp.float32) * deviation * loudness
    return jnp.minimum(jnp.maximum(values, -most), most).astype(kind)


def setup_inputs(seed: int = 0) -> dict:
    key_list = jax.random.split(jax.random.key(seed), 7)
    incoming = noise(key_list[0], (N_PP, TOKENS, D), 1.0, 6.0, ((0, 12), (1, 64)))
    expert_ids_keys = jax.random.split(jax.random.fold_in(key_list[1], 1), N_PP * TOKENS // TOK_DEV)
    expert_ids_turns = jax.random.permutation(jax.random.fold_in(key_list[1], 3), N_PP * TOKENS // TOK_DEV)
    expert_ids = jax.vmap(lambda own, number: deal_out(jax.random.fold_in(key_list[1], 2), own, number, TOK_DEV, EXPERTS, TOPK, CAP, 2))(expert_ids_keys, expert_ids_turns).reshape((N_PP, TOKENS, TOPK))
    gate_scores = jnp.clip(jnp.exp(math.log(1.0) - 2.9957323 * jax.random.uniform(key_list[2], (N_PP, TOKENS, TOPK), jnp.float32) ** steps_of(key_list[2], (N_PP, TOKENS, TOPK), ((0, 12), (1, 64)), -0.2, 0.2)), 0.05, 1.0)
    gate_proj = noise(key_list[3], (EXPERTS, D, FF), D ** -0.5, 0.125, ((0, 64),))
    up_proj = noise(key_list[4], (EXPERTS, D, FF), D ** -0.5, 0.125, ((0, 64),))
    down_proj = noise(key_list[5], (EXPERTS, FF, D), FF ** -0.5, 0.21875, ((0, 64),))
    return {"incoming": incoming, "expert_ids": expert_ids, "gate_scores": gate_scores, "gate_proj": gate_proj, "up_proj": up_proj, "down_proj": down_proj}


def expert_apply(tokens_in, gate_mat, up_mat, down_mat):
    gate_part = jnp.dot(tokens_in, gate_mat, preferred_element_type=jnp.float32)
    upward = jnp.dot(tokens_in, up_mat, preferred_element_type=jnp.float32)
    hidden = (jax.nn.silu(gate_part) * upward).astype(jnp.bfloat16)
    return jnp.dot(hidden, down_mat, preferred_element_type=jnp.float32).astype(jnp.bfloat16)

def reference(incoming, expert_ids, gate_scores, gate_proj, up_proj, down_proj):
    arrived = jnp.roll(incoming, 1, axis=0).reshape(-1, D)
    values = arrived.astype(jnp.float32)
    normed = (values * lax.rsqrt(lax.optimization_barrier(jnp.mean(values * values, axis=1, keepdims=True)) + 1e-06)).astype(jnp.bfloat16)
    token_total = values.shape[0]
    chosen = expert_ids.reshape(-1).astype(jnp.int32)
    scores = gate_scores.reshape(token_total, TOPK)
    weights = (scores / lax.optimization_barrier(jnp.sum(scores, axis=1, keepdims=True))).reshape(-1)
    assign_total = chosen.shape[0]
    ordering = jnp.argsort(chosen, stable=True).astype(jnp.int32)
    sorted_ids = chosen[ordering]
    counts = jnp.zeros((EXPERTS,), jnp.int32).at[chosen].add(1)
    starts = jnp.cumsum(counts).astype(jnp.int32) - counts
    position = jnp.arange(assign_total, dtype=jnp.int32) - starts[sorted_ids]
    row_bound = N_PP * N_TP * N_EP * CAP
    table_tok = jnp.full((EXPERTS, row_bound), token_total, jnp.int32).at[sorted_ids, position].set(ordering // TOPK)
    table_weight = jnp.zeros((EXPERTS, row_bound), jnp.float32).at[sorted_ids, position].set(weights[ordering])
    with_blank = jnp.concatenate([normed, jnp.zeros((1, D), jnp.bfloat16)], axis=0)

    def per_expert(summed, inputs):
        gate_mat, up_mat, down_mat, tok_list, weight_list = inputs
        answered = expert_apply(with_blank[tok_list], gate_mat, up_mat, down_mat)
        return (summed.at[tok_list].add(weight_list[:, None] * answered.astype(jnp.float32)), None)
    summed, unused = lax.scan(per_expert, jnp.zeros((token_total + 1, D), jnp.float32), (gate_proj, up_proj, down_proj, table_tok, table_weight))
    combined = values + summed[:token_total]
    return combined.astype(jnp.bfloat16).reshape(incoming.shape)
```

```python
import functools

import jax
import jax.numpy as jnp
from jax import lax
from jax.experimental import pallas as pl
from jax.experimental.pallas import tpu as pltpu
from jax.sharding import PartitionSpec as P

CHUNKS = 1
AXES = ("tp", "ep")
F32, BF16, I32 = jnp.float32, jnp.bfloat16, jnp.int32


def shifted(block, axis, distance):
    devices = range(lax.axis_size(axis))
    route = [((i - distance) % len(devices), i) for i in devices]
    return lax.ppermute(block, axis, route)


def iota(shape, dim):
    return lax.broadcasted_iota(I32, shape, dim)


def dispatch_kernel(experts, cap, ids_ref, x_ref, *refs):
    out_refs, normed_ref = refs[:-1], refs[-1]
    step = pl.program_id(0)

    @pl.when(step == 0)
    def _():
        values = x_ref[...].astype(F32)
        scale = lax.rsqrt(jnp.mean(values * values, axis=1, keepdims=True) + 1e-06)
        normed_ref[...] = (values * scale).astype(BF16)

    ids = ids_ref[...]
    tokens = ids.shape[1]
    named = ids[0:1, :] * 0 + step * experts + iota((experts, tokens), 0)
    member = (ids[0:1, :] == named) | (ids[1:2, :] == named)
    earlier = (iota((tokens, tokens), 0) < iota((tokens, tokens), 1)).astype(BF16)
    slot = jnp.dot(member.astype(BF16), earlier, preferred_element_type=F32).astype(I32)
    slot = jnp.where(member, slot, -1)
    pick = slot[:, None, :] == iota((experts, cap, tokens), 1)
    pick = pick.astype(F32).reshape(experts * cap, tokens).astype(BF16)
    width = out_refs[0].shape[1]
    for c, out_ref in enumerate(out_refs):
        rows = normed_ref[:, c * width : (c + 1) * width]
        out_ref[...] = jnp.dot(pick, rows, preferred_element_type=F32).astype(BF16)


def dispatch(ids, arrived, experts, cap, chunks, steps=4):
    tokens, features = arrived.shape
    width = features // chunks
    rows = experts * cap // steps
    return pl.pallas_call(
        functools.partial(dispatch_kernel, experts // steps, cap),
        grid=(steps,),
        in_specs=[
            pl.BlockSpec(ids.shape, lambda i: (0, 0)),
            pl.BlockSpec(arrived.shape, lambda i: (0, 0)),
        ],
        out_specs=[pl.BlockSpec((rows, width), lambda i: (i, 0))] * chunks,
        out_shape=[jax.ShapeDtypeStruct((experts * cap, width), BF16)] * chunks,
        scratch_shapes=[pltpu.VMEM((tokens, features), BF16)],
        name="dispatch",
    )(ids, arrived)


def combine_kernel(experts, cap, ids_ref, scores_ref, back_ref, x_ref, *refs):
    out_ref, pick_ref, weight_ref = refs[-3:]
    tokens = ids_ref.shape[1]
    square = (tokens, tokens)

    @pl.when(pl.program_id(0) == 0)
    def _():
        scores = scores_ref[...]
        weights = scores / jnp.sum(scores, axis=0, keepdims=True)
        ids = ids_ref[...].astype(F32)
        column = lambda a, k: jnp.transpose(jnp.broadcast_to(a[k : k + 1, :], square))
        names = [column(ids, k).astype(I32) for k in range(2)]
        lane = iota(square, 1)
        member = ((names[0] == lane) | (names[1] == lane)).astype(BF16)
        earlier = (iota(square, 1) < iota(square, 0)).astype(BF16)
        slot = jnp.dot(earlier, member, preferred_element_type=F32)
        for k in range(2):
            mine = jnp.sum(jnp.where(names[k] == lane, slot, 0.0), axis=1, keepdims=True)
            at = names[k][:, 0:1] * cap + mine.astype(I32)
            here = (iota((tokens, experts * cap), 1) == at).astype(BF16)
            pick_ref[k * tokens : (k + 1) * tokens, :] = here
            weight_ref[k * tokens : (k + 1) * tokens, :] = column(weights, k)

    picked = jnp.dot(pick_ref[...], back_ref[...], preferred_element_type=F32)
    picked = picked * weight_ref[:, 0:1]
    total = x_ref[...].astype(F32) + (picked[:tokens] + picked[tokens:])
    out_ref[...] = total.astype(BF16)


def combine(ids, scores, back, arrived, out, chunk, experts, cap, block=512):
    tokens, features = arrived.shape
    width = back.shape[1]
    base = chunk * width // block
    small = pl.BlockSpec(ids.shape, lambda i: (0, 0))
    place = pl.BlockSpec((tokens, block), lambda i: (0, base + i))
    operands = [ids, scores, back, arrived]
    specs = [small, small, pl.BlockSpec((experts * cap, block), lambda i: (0, i)), place]
    aliases = {}
    if out is not None:
        operands.append(out)
        specs.append(pl.BlockSpec(memory_space=pl.ANY))
        aliases = {4: 0}
    return pl.pallas_call(
        functools.partial(combine_kernel, experts, cap),
        grid=(width // block,),
        in_specs=specs,
        out_specs=place,
        out_shape=jax.ShapeDtypeStruct((tokens, features), BF16),
        scratch_shapes=[
            pltpu.VMEM((2 * tokens, experts * cap), BF16),
            pltpu.VMEM((2 * tokens, tokens), F32),
        ],
        input_output_aliases=aliases,
        name="combine",
    )(*operands)


def exchange(block, experts):
    shape = block.shape
    block = block.reshape(experts, -1, shape[1])
    block = lax.all_to_all(block, AXES, split_axis=0, concat_axis=0, tiled=True)
    return block.reshape(shape)


def shards(incoming, expert_ids, gate_scores, gate_proj, up_proj, down_proj):
    arrived = shifted(incoming, "pp", 1)[0]
    tokens, features = arrived.shape
    experts = lax.axis_size("tp") * lax.axis_size("ep")
    cap = min(tokens, 2 * tokens * expert_ids.shape[2] // experts)
    ids, scores = expert_ids[0].T, gate_scores[0].T
    width = features // CHUNKS
    outgoing = dispatch(ids, arrived, experts, cap, CHUNKS)
    gate = up = 0.0
    for c, block in enumerate(outgoing):
        rows = exchange(block, experts)
        part = slice(c * width, (c + 1) * width)
        gate = gate + jnp.dot(rows, gate_proj[0, part], preferred_element_type=F32)
        up = up + jnp.dot(rows, up_proj[0, part], preferred_element_type=F32)
    hidden = (jax.nn.silu(gate) * up).astype(BF16)
    out = None
    backs = []
    for c in range(CHUNKS):
        part = slice(c * width, (c + 1) * width)
        answered = jnp.dot(hidden, down_proj[0, :, part], preferred_element_type=F32)
        backs.append(exchange(answered.astype(BF16), experts))
    for c, back in enumerate(backs):
        out = combine(ids, scores, back, arrived, out, c, experts, cap)
    return out[None]


def solution(mesh):
    placed = (
        P("pp", ("tp", "ep"), None),
        P("pp", ("tp", "ep"), None),
        P("pp", ("tp", "ep"), None),
        P(("tp", "ep"), None, None),
        P(("tp", "ep"), None, None),
        P(("tp", "ep"), None, None),
    )
    return jax.shard_map(
        shards, mesh=mesh, in_specs=placed, out_specs=P("pp", ("tp", "ep"), None), check_vma=False
    )
```

```python
import functools

import jax
import jax.numpy as jnp
from jax import lax
from jax.experimental import pallas as pl
from jax.experimental.pallas import tpu as pltpu
from jax.sharding import Mesh
from jax.sharding import PartitionSpec as P

SAME_CORE = ("y", "ep")
F32, BF16, I32 = jnp.float32, jnp.bfloat16, jnp.int32


def iota(shape, dim):
    return lax.broadcasted_iota(I32, shape, dim)


def moved(block, planes, swap):
    count, cores = lax.axis_size("pp"), lax.axis_size("core")
    route = []
    for p in range(count):
        for c in range(cores):
            to = ((p + planes) % count) * cores + (cores - 1 - c if swap else c)
            route.append((p * cores + c, to))
    return lax.ppermute(block, ("pp", "core"), route)


def route_kernel(width, core_ref, ids_ref, scores_ref, other_ref, own_ref):
    ids, scores = ids_ref[...], scores_ref[...]
    weights = scores / jnp.sum(scores, axis=0, keepdims=True)
    core = core_ref[0]
    half = (ids // width) % 2
    place = (ids // (2 * width)) * width + ids % width
    for ref, mine in ((other_ref, 1 - core), (own_ref, core)):
        ref[0:2, :] = jnp.where(half == mine, place, -1).astype(F32)
        ref[2:4, :] = weights


def route(ids, scores, width):
    core = lax.axis_index("core").astype(I32).reshape(1)
    shape = jax.ShapeDtypeStruct((4, ids.shape[1]), F32)
    vmem = pl.BlockSpec(memory_space=pltpu.VMEM)
    return pl.pallas_call(
        functools.partial(route_kernel, width),
        in_specs=[pl.BlockSpec(memory_space=pltpu.SMEM), vmem, vmem],
        out_specs=[vmem, vmem],
        out_shape=[shape, shape],
        name="route",
    )(core, ids, scores)


def dispatch_kernel(experts, cap, route_ref, x_ref, out_ref, normed_ref):
    step = pl.program_id(0)

    @pl.when(step == 0)
    def _():
        values = x_ref[...].astype(F32)
        scale = lax.rsqrt(jnp.mean(values * values, axis=1, keepdims=True) + 1e-06)
        normed_ref[...] = (values * scale).astype(BF16)

    names = route_ref[0:2, :].astype(I32)
    tokens = names.shape[1]
    place = step * experts + iota((experts, tokens), 0)
    member = (names[0:1, :] == place) | (names[1:2, :] == place)
    earlier = (iota((tokens, tokens), 0) < iota((tokens, tokens), 1)).astype(BF16)
    slot = jnp.dot(member.astype(BF16), earlier, preferred_element_type=F32).astype(I32)
    slot = jnp.where(member, slot, -1)
    pick = slot[:, None, :] == iota((experts, cap, tokens), 1)
    pick = pick.astype(F32).reshape(experts * cap, tokens).astype(BF16)
    out_ref[...] = jnp.dot(pick, normed_ref[...], preferred_element_type=F32).astype(BF16)


def dispatch(routed, arrived, experts, cap, steps=2):
    tokens, features = arrived.shape
    rows = experts * cap // steps
    return pl.pallas_call(
        functools.partial(dispatch_kernel, experts // steps, cap),
        grid=(steps,),
        in_specs=[
            pl.BlockSpec(routed.shape, lambda i: (0, 0)),
            pl.BlockSpec(arrived.shape, lambda i: (0, 0)),
        ],
        out_specs=pl.BlockSpec((rows, features), lambda i: (i, 0)),
        out_shape=jax.ShapeDtypeStruct((experts * cap, features), BF16),
        scratch_shapes=[pltpu.VMEM((tokens, features), BF16)],
        cost_estimate=pl.CostEstimate(
            flops=2 * experts * cap * tokens * features,
            bytes_accessed=2 * features * (tokens + experts * cap),
            transcendentals=0,
        ),
        name="dispatch",
    )(routed, arrived)


def combine_kernel(experts, cap, route_ref, back_ref, x_ref, out_ref, pick_ref, weight_ref):
    tokens = route_ref.shape[1]
    square = (tokens, tokens)

    @pl.when(pl.program_id(0) == 0)
    def _():
        column = lambda k: jnp.transpose(jnp.broadcast_to(route_ref[k : k + 1, :], square))
        names = [column(k).astype(I32) for k in range(2)]
        lane = iota(square, 1)
        member = ((names[0] == lane) | (names[1] == lane)).astype(BF16)
        earlier = (iota(square, 1) < iota(square, 0)).astype(BF16)
        slot = jnp.dot(earlier, member, preferred_element_type=F32)
        for k in range(2):
            mine = jnp.sum(jnp.where(names[k] == lane, slot, 0.0), axis=1, keepdims=True)
            at = names[k][:, 0:1] * cap + mine.astype(I32)
            here = (iota((tokens, experts * cap), 1) == at).astype(BF16)
            pick_ref[k * tokens : (k + 1) * tokens, :] = here
            weight_ref[k * tokens : (k + 1) * tokens, :] = column(2 + k)

    picked = jnp.dot(pick_ref[...], back_ref[...], preferred_element_type=F32)
    picked = picked * weight_ref[:, 0:1]
    total = x_ref[...].astype(F32) + (picked[:tokens] + picked[tokens:])
    out_ref[...] = total.astype(BF16)


def combine(routed, back, base, experts, cap, block=512):
    tokens, features = base.shape
    column = lambda rows: pl.BlockSpec((rows, block), lambda i: (0, i))
    return pl.pallas_call(
        functools.partial(combine_kernel, experts, cap),
        grid=(features // block,),
        in_specs=[
            pl.BlockSpec(routed.shape, lambda i: (0, 0)),
            column(experts * cap),
            column(tokens),
        ],
        out_specs=column(tokens),
        out_shape=jax.ShapeDtypeStruct((tokens, features), BF16),
        scratch_shapes=[
            pltpu.VMEM((2 * tokens, experts * cap), BF16),
            pltpu.VMEM((2 * tokens, tokens), F32),
        ],
        cost_estimate=pl.CostEstimate(
            flops=4 * experts * cap * tokens * features,
            bytes_accessed=2 * features * (2 * tokens + experts * cap),
            transcendentals=0,
        ),
        name="combine",
    )(routed, back, base)


def exchange(block, experts):
    shape = block.shape
    block = block.reshape(experts, -1, shape[1])
    block = lax.all_to_all(block, SAME_CORE, split_axis=0, concat_axis=0, tiled=True)
    return block.reshape(shape)


def expert_apply(tokens_in, gate_mat, up_mat, down_mat):
    gate_part = jnp.dot(tokens_in, gate_mat, preferred_element_type=F32)
    upward = jnp.dot(tokens_in, up_mat, preferred_element_type=F32)
    hidden = (jax.nn.silu(gate_part) * upward).astype(BF16)
    return jnp.dot(hidden, down_mat, preferred_element_type=F32).astype(BF16)


def shards(incoming, expert_ids, gate_scores, gate_proj, up_proj, down_proj):
    leaving = incoming[0]
    tokens, _ = leaving.shape
    columns = lax.axis_size("ep")
    experts = lax.axis_size("y") * columns
    cap = min(tokens, tokens * expert_ids.shape[2] // experts)
    weights = (gate_proj[0], up_proj[0], down_proj[0])
    other, own = route(expert_ids[0].T, gate_scores[0].T, columns)
    asked = moved(other, -1, True)
    swapped = moved(leaving, 0, True)
    arrived = moved(leaving, 1, False)
    first = dispatch(asked, swapped, experts, cap)
    first = exchange(first, experts)
    second = dispatch(own, arrived, experts, cap)
    second = exchange(second, experts)
    first = expert_apply(first, *weights)
    first = exchange(first, experts)
    second = expert_apply(second, *weights)
    second = exchange(second, experts)
    partial = combine(asked, first, swapped, experts, cap)
    partial = moved(partial, 1, True)
    out = combine(own, second, partial, experts, cap)
    return out[None]


def solution(mesh):
    planes, rows, columns = mesh.devices.shape
    devices = mesh.devices.reshape(planes, rows // 2, 2, columns)
    fine = Mesh(devices, ("pp", "y", "core", "ep"))
    spread = ("y", "core", "ep")
    placed = (P("pp", spread, None),) * 3 + (P(spread, None, None),) * 3
    return jax.shard_map(
        shards, mesh=fine, in_specs=placed, out_specs=P("pp", spread, None), check_vma=False
    )
```

```python
import functools

import jax
import jax.numpy as jnp
from jax import lax
from jax.experimental import pallas as pl
from jax.experimental.pallas import tpu as pltpu
from jax.sharding import Mesh
from jax.sharding import PartitionSpec as P

SAME_CORE = ("y", "ep")
F32, BF16, I32 = jnp.float32, jnp.bfloat16, jnp.int32


def iota(shape, dim):
    return lax.broadcasted_iota(I32, shape, dim)


def moved(block, planes, swap):
    count, cores = lax.axis_size("pp"), lax.axis_size("core")
    route = []
    for p in range(count):
        for c in range(cores):
            to = ((p + planes) % count) * cores + (cores - 1 - c if swap else c)
            route.append((p * cores + c, to))
    return lax.ppermute(block, ("pp", "core"), route)


def places(ids, width, core):
    place = lax.div(ids, 2 * width) * width + lax.rem(ids, width)
    return jnp.where(lax.rem(lax.div(ids, width), 2) == core, place, -1)


def dispatch_kernel(experts, cap, width, core_ref, ids_ref, x_ref, out_ref, normed_ref):
    step = pl.program_id(0)

    @pl.when(step == 0)
    def _():
        values = x_ref[...].astype(F32)
        scale = lax.rsqrt(jnp.mean(values * values, axis=1, keepdims=True) + 1e-06)
        normed_ref[...] = (values * scale).astype(BF16)

    names = places(ids_ref[...], width, core_ref[0])
    tokens = names.shape[1]
    place = step * experts + iota((experts, tokens), 0)
    member = (names[0:1, :] == place) | (names[1:2, :] == place)
    earlier = (iota((tokens, tokens), 0) < iota((tokens, tokens), 1)).astype(BF16)
    slot = jnp.dot(member.astype(BF16), earlier, preferred_element_type=F32).astype(I32)
    slot = jnp.where(member, slot, -1)
    pick = slot[:, None, :] == iota((experts, cap, tokens), 1)
    pick = pick.astype(F32).reshape(experts * cap, tokens).astype(BF16)
    out_ref[...] = jnp.dot(pick, normed_ref[...], preferred_element_type=F32).astype(BF16)


def dispatch(core, ids, arrived, experts, cap, width, steps=1):
    tokens, features = arrived.shape
    rows = experts * cap // steps
    return pl.pallas_call(
        functools.partial(dispatch_kernel, experts // steps, cap, width),
        grid=(steps,),
        in_specs=[
            pl.BlockSpec(memory_space=pltpu.SMEM),
            pl.BlockSpec(memory_space=pltpu.VMEM),
            pl.BlockSpec(arrived.shape, lambda i: (0, 0)),
        ],
        out_specs=pl.BlockSpec((rows, features), lambda i: (i, 0)),
        out_shape=jax.ShapeDtypeStruct((experts * cap, features), BF16),
        scratch_shapes=[pltpu.VMEM((tokens, features), BF16)],
        cost_estimate=pl.CostEstimate(
            flops=2 * experts * cap * tokens * features,
            bytes_accessed=2 * features * (tokens + experts * cap),
            transcendentals=0,
        ),
        name="dispatch",
    )(core, ids, arrived)


def lookup_kernel(experts, cap, width, other, core_ref, ids_ref, scores_ref, _, pick_ref, weight_ref):
    core = 1 - core_ref[0] if other else core_ref[0]
    tokens = ids_ref.shape[1]
    square = (tokens, tokens)
    column = lambda row: jnp.transpose(jnp.broadcast_to(row, square))
    scores = scores_ref[...]
    weights = scores / jnp.sum(scores, axis=0, keepdims=True)
    names = places(ids_ref[...], width, core).astype(F32)
    names = [column(names[k : k + 1, :]).astype(I32) for k in range(2)]
    lane = iota(square, 1)
    member = ((names[0] == lane) | (names[1] == lane)).astype(BF16)
    earlier = (iota(square, 1) < iota(square, 0)).astype(BF16)
    slot = jnp.dot(earlier, member, preferred_element_type=F32)
    for k in range(2):
        mine = jnp.sum(jnp.where(names[k] == lane, slot, 0.0), axis=1, keepdims=True)
        at = names[k][:, 0:1] * cap + mine.astype(I32)
        rows = slice(k * tokens, (k + 1) * tokens)
        pick_ref[rows, :] = (iota((tokens, experts * cap), 1) == at).astype(BF16)
        weight_ref[rows, :] = column(weights[k : k + 1, :])


def lookup(core, ids, scores, after, experts, cap, width, other):
    tokens = ids.shape[1]
    vmem = pl.BlockSpec(memory_space=pltpu.VMEM)
    return pl.pallas_call(
        functools.partial(lookup_kernel, experts, cap, width, other),
        in_specs=[
            pl.BlockSpec(memory_space=pltpu.SMEM),
            vmem,
            vmem,
            pl.BlockSpec(memory_space=pl.ANY),
        ],
        out_specs=[vmem, vmem],
        out_shape=[
            jax.ShapeDtypeStruct((2 * tokens, experts * cap), BF16),
            jax.ShapeDtypeStruct((2 * tokens, tokens), F32),
        ],
        name="lookup",
    )(core, ids, scores, after)


def combine_kernel(tokens, pick_ref, weight_ref, back_ref, x_ref, out_ref):
    picked = jnp.dot(pick_ref[...], back_ref[...], preferred_element_type=F32)
    picked = picked * weight_ref[:, 0:1]
    total = x_ref[...].astype(F32) + (picked[:tokens] + picked[tokens:])
    out_ref[...] = total.astype(BF16)


def combine(found, back, base, block=1024):
    pick, weight = found
    tokens, features = base.shape
    rows = back.shape[0]
    column = lambda count: pl.BlockSpec((count, block), lambda i: (0, i))
    return pl.pallas_call(
        functools.partial(combine_kernel, tokens),
        grid=(features // block,),
        in_specs=[
            pl.BlockSpec(pick.shape, lambda i: (0, 0)),
            pl.BlockSpec(weight.shape, lambda i: (0, 0)),
            column(rows),
            column(tokens),
        ],
        out_specs=column(tokens),
        out_shape=jax.ShapeDtypeStruct((tokens, features), BF16),
        cost_estimate=pl.CostEstimate(
            flops=4 * rows * tokens * features,
            bytes_accessed=2 * features * (2 * tokens + rows),
            transcendentals=0,
        ),
        name="combine",
    )(pick, weight, back, base)


def exchange(block, experts):
    shape = block.shape
    block = block.reshape(experts, -1, shape[1])
    block = lax.all_to_all(block, SAME_CORE, split_axis=0, concat_axis=0, tiled=True)
    return block.reshape(shape)


def expert_apply(tokens_in, gate_mat, up_mat, down_mat):
    gate_part = jnp.dot(tokens_in, gate_mat, preferred_element_type=F32)
    upward = jnp.dot(tokens_in, up_mat, preferred_element_type=F32)
    hidden = (jax.nn.silu(gate_part) * upward).astype(BF16)
    return jnp.dot(hidden, down_mat, preferred_element_type=F32).astype(BF16)


def shards(incoming, expert_ids, gate_scores, gate_proj, up_proj, down_proj):
    leaving = incoming[0]
    tokens, _ = leaving.shape
    columns = lax.axis_size("ep")
    experts = lax.axis_size("y") * columns
    cap = min(tokens, tokens * expert_ids.shape[2] // experts)
    weights = (gate_proj[0], up_proj[0], down_proj[0])
    core = lax.axis_index("core").astype(I32).reshape(1)
    ids, scores = expert_ids[0].T, gate_scores[0].T
    sizes = (experts, cap, columns)
    asked = moved(ids, -1, False)
    first = dispatch(core, asked, leaving, *sizes)
    first, ids_b, scores_b = lax.optimization_barrier((first, ids, scores))
    first = exchange(first, experts)
    arrived = moved(leaving, 1, True)
    beside = moved(ids_b, 0, True)
    asked_scores = moved(scores_b, -1, False)
    second = dispatch(core, beside, arrived, *sizes)
    second = exchange(second, experts)
    found1 = lookup(core, asked, asked_scores, arrived, *sizes, False)
    found2 = lookup(core, ids, scores, arrived, *sizes, True)
    first = expert_apply(first, *weights)
    first, found1, found2 = lax.optimization_barrier((first, found1, found2))
    first = exchange(first, experts)
    second = expert_apply(second, *weights)
    second = moved(second, 0, True)
    second = exchange(second, experts)
    partial = combine(found1, first, leaving)
    partial = moved(partial, 1, False)
    out = combine(found2, second, partial)
    return out[None]


def solution(mesh):
    planes, rows, columns = mesh.devices.shape
    devices = mesh.devices.reshape(planes, rows // 2, 2, columns)
    fine = Mesh(devices, ("pp", "y", "core", "ep"))
    spread = ("y", "core", "ep")
    placed = (P("pp", spread, None),) * 3 + (P(spread, None, None),) * 3
    return jax.shard_map(
        shards, mesh=fine, in_specs=placed, out_specs=P("pp", spread, None), check_vma=False
    )
```

```python
import functools

import jax
import jax.numpy as jnp
from jax import lax
from jax.experimental import pallas as pl
from jax.experimental.pallas import tpu as pltpu
from jax.sharding import Mesh
from jax.sharding import PartitionSpec as P

SAME_CORE = ("y", "ep")
VMEM_LIMIT = 12 << 20
F32, BF16, I32 = jnp.float32, jnp.bfloat16, jnp.int32


def iota(shape, dim):
    return lax.broadcasted_iota(I32, shape, dim)


def moved(block, planes, swap):
    count, cores = lax.axis_size("pp"), lax.axis_size("core")
    route = []
    for p in range(count):
        for c in range(cores):
            to = ((p + planes) % count) * cores + (cores - 1 - c if swap else c)
            route.append((p * cores + c, to))
    return lax.ppermute(block, ("pp", "core"), route)


def places(ids, width, core):
    place = lax.div(ids, 2 * width) * width + lax.rem(ids, width)
    return jnp.where(lax.rem(lax.div(ids, width), 2) == core, place, -1)


def norm_kernel(x_ref, out_ref):
    values = x_ref[...].astype(F32)
    scale = lax.rsqrt(jnp.mean(values * values, axis=1, keepdims=True) + 1e-06)
    out_ref[...] = (values * scale).astype(BF16)


def norm(x):
    return pl.pallas_call(
        norm_kernel,
        out_shape=jax.ShapeDtypeStruct(x.shape, BF16),
        cost_estimate=pl.CostEstimate(
            flops=4 * x.size, bytes_accessed=4 * x.size, transcendentals=x.shape[0]
        ),
        compiler_params=pltpu.CompilerParams(vmem_limit_bytes=VMEM_LIMIT),
        name="norm",
    )(x)


def dispatch_kernel(experts, cap, width, core_ref, ids_ref, normed_ref, out_ref):
    names = places(ids_ref[...], width, core_ref[0])
    tokens = names.shape[1]
    place = iota((experts, tokens), 0)
    member = (names[0:1, :] == place) | (names[1:2, :] == place)
    earlier = (iota((tokens, tokens), 0) < iota((tokens, tokens), 1)).astype(BF16)
    slot = jnp.dot(member.astype(BF16), earlier, preferred_element_type=F32).astype(I32)
    slot = jnp.where(member, slot, -1)
    pick = slot[:, None, :] == iota((experts, cap, tokens), 1)
    pick = pick.astype(F32).reshape(experts * cap, tokens).astype(BF16)
    out_ref[...] = jnp.dot(pick, normed_ref[...], preferred_element_type=F32).astype(BF16)


def dispatch(core, ids, normed, experts, cap, width):
    tokens, features = normed.shape
    vmem = pl.BlockSpec(memory_space=pltpu.VMEM)
    return pl.pallas_call(
        functools.partial(dispatch_kernel, experts, cap, width),
        in_specs=[pl.BlockSpec(memory_space=pltpu.SMEM), vmem, vmem],
        out_specs=vmem,
        out_shape=jax.ShapeDtypeStruct((experts * cap, features), BF16),
        cost_estimate=pl.CostEstimate(
            flops=2 * experts * cap * tokens * features,
            bytes_accessed=2 * features * (tokens + experts * cap),
            transcendentals=0,
        ),
        compiler_params=pltpu.CompilerParams(vmem_limit_bytes=VMEM_LIMIT),
        name="dispatch",
    )(core, ids, normed)


def lookup_kernel(experts, cap, width, other, core_ref, ids_ref, scores_ref, _, pick_ref, weight_ref):
    core = 1 - core_ref[0] if other else core_ref[0]
    tokens = ids_ref.shape[1]
    square = (tokens, tokens)
    column = lambda row: jnp.transpose(jnp.broadcast_to(row, square))
    scores = scores_ref[...]
    weights = scores / jnp.sum(scores, axis=0, keepdims=True)
    names = places(ids_ref[...], width, core).astype(F32)
    names = [column(names[k : k + 1, :]).astype(I32) for k in range(2)]
    lane = iota(square, 1)
    member = ((names[0] == lane) | (names[1] == lane)).astype(BF16)
    earlier = (iota(square, 1) < iota(square, 0)).astype(BF16)
    slot = jnp.dot(earlier, member, preferred_element_type=F32)
    for k in range(2):
        mine = jnp.sum(jnp.where(names[k] == lane, slot, 0.0), axis=1, keepdims=True)
        at = names[k][:, 0:1] * cap + mine.astype(I32)
        rows = slice(k * tokens, (k + 1) * tokens)
        pick_ref[rows, :] = (iota((tokens, experts * cap), 1) == at).astype(BF16)
        weight_ref[rows, :] = column(weights[k : k + 1, :])


def lookup(core, ids, scores, after, experts, cap, width, other):
    tokens = ids.shape[1]
    vmem = pl.BlockSpec(memory_space=pltpu.VMEM)
    return pl.pallas_call(
        functools.partial(lookup_kernel, experts, cap, width, other),
        in_specs=[
            pl.BlockSpec(memory_space=pltpu.SMEM),
            vmem,
            vmem,
            pl.BlockSpec(memory_space=pl.ANY),
        ],
        out_specs=[vmem, vmem],
        out_shape=[
            jax.ShapeDtypeStruct((2 * tokens, experts * cap), BF16),
            jax.ShapeDtypeStruct((2 * tokens, tokens), F32),
        ],
        compiler_params=pltpu.CompilerParams(vmem_limit_bytes=VMEM_LIMIT),
        name="lookup",
    )(core, ids, scores, after)


def combine_kernel(tokens, pick_ref, weight_ref, back_ref, x_ref, out_ref):
    picked = jnp.dot(pick_ref[...], back_ref[...], preferred_element_type=F32)
    picked = picked * weight_ref[:, 0:1]
    total = x_ref[...].astype(F32) + (picked[:tokens] + picked[tokens:])
    out_ref[...] = total.astype(BF16)


def combine(found, back, base, block=2048):
    pick, weight = found
    tokens, features = base.shape
    rows = back.shape[0]
    column = lambda count: pl.BlockSpec((count, block), lambda i: (0, i))
    return pl.pallas_call(
        functools.partial(combine_kernel, tokens),
        grid=(features // block,),
        in_specs=[
            pl.BlockSpec(pick.shape, lambda i: (0, 0)),
            pl.BlockSpec(weight.shape, lambda i: (0, 0)),
            column(rows),
            column(tokens),
        ],
        out_specs=column(tokens),
        out_shape=jax.ShapeDtypeStruct((tokens, features), BF16),
        cost_estimate=pl.CostEstimate(
            flops=4 * rows * tokens * features,
            bytes_accessed=2 * features * (2 * tokens + rows),
            transcendentals=0,
        ),
        compiler_params=pltpu.CompilerParams(vmem_limit_bytes=VMEM_LIMIT),
        name="combine",
    )(pick, weight, back, base)


def exchange(block, experts):
    shape = block.shape
    block = block.reshape(experts, -1, shape[1])
    block = lax.all_to_all(block, SAME_CORE, split_axis=0, concat_axis=0, tiled=True)
    return block.reshape(shape)


def expert_kernel(x_ref, gate_ref, up_ref, down_ref, out_ref, total_ref):
    step = pl.program_id(0)
    x = x_ref[...]
    gate = jnp.dot(x, gate_ref[...], preferred_element_type=F32)
    up = jnp.dot(x, up_ref[...], preferred_element_type=F32)
    hidden = (gate / (1.0 + jnp.exp(-gate)) * up).astype(BF16)
    part = jnp.dot(hidden, down_ref[...], preferred_element_type=F32)

    @pl.when(step == 0)
    def _():
        total_ref[...] = part

    @pl.when(step > 0)
    def _():
        total_ref[...] += part

    @pl.when(step == pl.num_programs(0) - 1)
    def _():
        out_ref[...] = total_ref[...].astype(BF16)


def expert_apply(rows, gate_mat, up_mat, down_mat, block=256):
    count, features = rows.shape
    hidden = gate_mat.shape[1]
    whole = pl.BlockSpec((count, features), lambda i: (0, 0))
    return pl.pallas_call(
        expert_kernel,
        grid=(hidden // block,),
        in_specs=[
            whole,
            pl.BlockSpec((features, block), lambda i: (0, i)),
            pl.BlockSpec((features, block), lambda i: (0, i)),
            pl.BlockSpec((block, features), lambda i: (i, 0)),
        ],
        out_specs=whole,
        out_shape=jax.ShapeDtypeStruct((count, features), BF16),
        scratch_shapes=[pltpu.VMEM((count, features), F32)],
        cost_estimate=pl.CostEstimate(
            flops=6 * count * features * hidden,
            bytes_accessed=2 * (3 * features * hidden + 2 * count * features),
            transcendentals=count * hidden,
        ),
        compiler_params=pltpu.CompilerParams(vmem_limit_bytes=2 * VMEM_LIMIT),
        name="expert",
    )(rows, gate_mat, up_mat, down_mat)


def shards(incoming, expert_ids, gate_scores, gate_proj, up_proj, down_proj):
    leaving = incoming[0]
    tokens, _ = leaving.shape
    columns = lax.axis_size("ep")
    experts = lax.axis_size("y") * columns
    cap = min(tokens, tokens * expert_ids.shape[2] // experts)
    weights = (gate_proj[0], up_proj[0], down_proj[0])
    core = lax.axis_index("core").astype(I32).reshape(1)
    ids, scores = expert_ids[0].T, gate_scores[0].T
    sizes = (experts, cap, columns)
    asked = moved(ids, -1, False)
    normed = norm(leaving)
    first = dispatch(core, asked, normed, *sizes)
    first, ids_b, scores_b = lax.optimization_barrier((first, ids, scores))
    first = exchange(first, experts)
    arrived = moved(leaving, 1, True)
    beside = moved(ids_b, 0, True)
    asked_scores = moved(scores_b, -1, False)
    second = dispatch(core, beside, norm(arrived), *sizes)
    second = exchange(second, experts)
    found1 = lookup(core, asked, asked_scores, arrived, *sizes, False)
    found2 = lookup(core, ids, scores, arrived, *sizes, True)
    first = expert_apply(first, *weights)
    first, found1, found2 = lax.optimization_barrier((first, found1, found2))
    first = exchange(first, experts)
    second = expert_apply(second, *weights)
    second = moved(second, 0, True)
    second = exchange(second, experts)
    partial = combine(found1, first, leaving)
    partial = moved(partial, 1, False)
    out = combine(found2, second, partial)
    return out[None]


def solution(mesh):
    planes, rows, columns = mesh.devices.shape
    devices = mesh.devices.reshape(planes, rows // 2, 2, columns)
    fine = Mesh(devices, ("pp", "y", "core", "ep"))
    spread = ("y", "core", "ep")
    placed = (P("pp", spread, None),) * 3 + (P(spread, None, None),) * 3
    return jax.shard_map(
        shards, mesh=fine, in_specs=placed, out_specs=P("pp", spread, None), check_vma=False
    )
```
